128 devices in a mesh: expert: 16 (over y, x_hi, core), replica: 8 (over z, x_lo).
Axes of the slice: x: 4 (x_hi: 2, x_lo: 2; x = x_hi * 2 + x_lo), y: 4, z: 4, core: 2. Of those that a mesh axis runs over, the one named last changes fastest.
Arguments:
- tokens_in: bfloat16 [32768, 2048], P(('expert', 'replica')), may hold values from -6 to 6
- cotangents: bfloat16 [32768, 8192], P(('expert', 'replica')), may hold values from -0.1796875 to 0.1796875
- left_root: bfloat16 [16, 2048, 2048], P('expert'), may hold values from -2 to 6, as said below
- right_root: bfloat16 [16, 8, 1024, 1024], P('expert', 'replica'), may hold values from -2 to 6, as said below
Outputs:
- update: bfloat16 [16, 2048, 8192], P('expert', None, 'replica')
The draws below stay inside these ranges and needn't reach their ends.
Inputs may be any that keep to these rules, and one draw needn't show every extreme that they name: `left_root`: each matrix is symmetric. `right_root`: each block is symmetric.
All inputs are finite; a program needn't handle non-finite values.
Results may differ from the reference program's by a relative error of at most 0.0058.
Values may be sent and summed in bfloat16 or wider, within the bound.
A program may use at most 192 MiB of HBM per device.

```python
import math
import jax
import jax.numpy as jnp
from jax import lax

D = 2048
FF = 8192
BLOCK = 1024
EXPERTS = 16
SLOTS = 16
TOKENS = 32768
BLOCKS = 8


def factor_draw(key, leading, order):
    diag_key, noise_key = jax.random.split(key)
    diagonal = jnp.exp(jax.random.uniform(diag_key, leading + (order,), jnp.float32, 0.0, math.log(3.0)))
    random_part = jnp.clip(jax.random.normal(noise_key, leading + (order, order), jnp.float32), -4.0, 4.0)
    random_part = random_part * (0.8 / math.sqrt(order))
    symmetric = 0.5 * (random_part + jnp.swapaxes(random_part, -1, -2))
    identity = jnp.eye(order, dtype=jnp.float32)
    return (symmetric + identity * diagonal[..., None]).astype(jnp.bfloat16)


def draw_left_root(key, part):
    return factor_draw(jax.random.fold_in(key, 11), (EXPERTS,), D)


def draw_right_root(key, part):
    return factor_draw(jax.random.fold_in(key, 12), (EXPERTS, BLOCKS), BLOCK)


def block_scale(rng, dims, cuts, smallest, top_value):
    loudness = 1.0
    for position, shards_of in cuts:
        steps = jax.random.uniform(jax.random.fold_in(jax.random.fold_in(rng, 6), position), (shards_of,), jnp.float32, smallest / len(cuts), top_value / len(cuts))
        loudness = loudness * jnp.repeat(jnp.exp(steps), dims[position] // shards_of).reshape((-1,) + (1,) * (len(dims) - 1 - position))
    return loudness


def centred(stream_key, dims, spread, most, shards=(), kind=jnp.bfloat16):
    values = jax.random.normal(stream_key, dims, jnp.float32) * spread
    if len(shards) > 0:
        values = block_scale(stream_key, dims, shards, -0.22, 0.18) * values
    return jnp.clip(values, min=-most, max=most).astype(kind)


def setup_inputs(seed: int = 0) -> dict:
    streams_of = jax.random.split(jax.random.key(seed), 5)
    return {
        "tokens_in": centred(streams_of[0], (TOKENS, D), 1.0, 6.0, ((0, 128),)),
        "cotangents": centred(streams_of[1], (TOKENS, FF), 0.03, 0.1796875, ((0, 128),)),
        "left_root": draw_left_root(jax.random.fold_in(streams_of[4], 71), 0),
        "right_root": draw_right_root(jax.random.fold_in(streams_of[4], 71), 0),
    }


def per_expert(inputs):
    expert_tokens, expert_cotangents, left_factor, right_factor = inputs
    gradient = jnp.dot(expert_tokens.T, expert_cotangents, preferred_element_type=jnp.float32).astype(jnp.bfloat16)
    blocks = gradient.reshape(D, BLOCKS, BLOCK).astype(jnp.float32)
    applied = jnp.einsum("dbk,bkj->dbj", blocks, right_factor.astype(jnp.float32))
    applied = applied.astype(jnp.bfloat16).reshape(D, FF)
    return jnp.dot(left_factor, applied, preferred_element_type=jnp.float32).astype(jnp.bfloat16)


def reference(tokens_in, cotangents, left_root, right_root):
    token_groups = jnp.moveaxis(tokens_in.reshape(-1, EXPERTS, SLOTS, D), 1, 0).reshape(EXPERTS, -1, D)
    cotangent_groups = jnp.moveaxis(cotangents.reshape(-1, EXPERTS, SLOTS, FF), 1, 0).reshape(EXPERTS, -1, FF)
    return lax.map(per_expert, (token_groups, cotangent_groups, left_root, right_root))
```

```python
import jax
import jax.numpy as jnp
from jax import lax
from jax.experimental import pallas as pl
from jax.experimental.pallas import tpu as pltpu
from jax.sharding import PartitionSpec as P

MESH = pl.DeviceIdType.MESH
SLOTS = 16
BOTH = ("expert", "replica")


def position():
    e, r = lax.axis_index("expert"), lax.axis_index("replica")
    return ((e // 2) % 2) * 2 + r % 2, e // 4, r // 2, e % 2


def device(x, y, z, c):
    return (y * 2 + x // 2) * 2 + c, z * 2 + x % 2


def near(x, half):
    other = (x // 2 - half) * (x // 2 - half)
    return x + other * (3 - 2 * x)


def enter(plane_sem, all_sem):
    x, y, z, c = position()
    barrier = pltpu.get_barrier_semaphore()

    def greet(k, _):
        half, up, core = k % 2, (k // 2) % 4, k // 8
        to = device(x + half * (3 - 2 * x), (y + up) % 4, z, (c + core) % 2)
        pl.semaphore_signal(barrier, inc=1, device_id=to, device_id_type=MESH)
        return 0

    lax.fori_loop(1, 16, greet, 0)
    for up in (1, 2, 3):
        pl.semaphore_signal(barrier, inc=1, device_id=device(x, y, (z + up) % 4, c), device_id_type=MESH)
    beside = x + 1 - 2 * (x % 2)
    pl.semaphore_signal(barrier, inc=1, device_id=device(beside, y, z, c), device_id_type=MESH)
    pl.semaphore_wait(barrier, 19)


def enter_all(plane_sem, all_sem):
    x, y, z, c = position()
    for up in (1, 2, 3):
        pl.semaphore_signal(plane_sem, inc=1, device_id=device(x, y, (z + up) % 4, c), device_id_type=MESH)
    pl.semaphore_wait(plane_sem, 3)
    beside = x + 1 - 2 * (x % 2)
    pl.semaphore_signal(all_sem, inc=1, device_id=device(beside, y, z, c), device_id_type=MESH)
    pl.semaphore_wait(all_sem, 1)


def exchange(tok, cot, tok_out, cot_out, send, recv, csend, crecv, plane_sem, all_sem):
    x, y, z, c = position()
    e, r = lax.axis_index("expert"), lax.axis_index("replica")
    columns = cot_out.shape[1]
    place = ((y * 2 + c) * 2 + x // 2) * SLOTS
    enter(plane_sem, all_sem)
    pltpu.make_async_copy(tok.at[pl.ds(e * SLOTS, SLOTS)], tok_out.at[pl.ds(place, SLOTS)], recv).start()

    def send_tokens(k, _):
        half, up, core = k % 2, (k // 2) % 4, k // 8
        to = device(x + half * (3 - 2 * x), (y + up) % 4, z, (c + core) % 2)
        pltpu.make_async_remote_copy(
            tok.at[pl.ds(to[0] * SLOTS, SLOTS)], tok_out.at[pl.ds(place, SLOTS)],
            send, recv, device_id=to, device_id_type=MESH,
        ).start()
        return 0

    lax.fori_loop(1, 16, send_tokens, 0)
    enter_all(plane_sem, all_sem)

    def target(half):
        return (z * 2 + near(x, half) % 2) * 16 * SLOTS + place

    pltpu.make_async_copy(
        cot.at[pl.ds(e * SLOTS, SLOTS), pl.ds(r * columns, columns)],
        cot_out.at[pl.ds(target(x // 2), SLOTS)], crecv,
    ).start()

    def send_cotangents(k, _):
        a, b, d = k % 4, (k // 4) % 4, (k // 16) % 4
        tx = (x + a) % 4
        to = device(tx, (y + a + b) % 4, (z + a + d) % 4, (c + k // 64) % 2)
        pltpu.make_async_remote_copy(
            cot.at[pl.ds(to[0] * SLOTS, SLOTS), pl.ds(to[1] * columns, columns)],
            cot_out.at[pl.ds(target(tx // 2), SLOTS)],
            csend, crecv, device_id=to, device_id_type=MESH,
        ).start()
        return 0

    lax.fori_loop(1, 128, send_cotangents, 0)
    pltpu.make_async_copy(tok_out, tok_out, recv).wait()
    most = tok_out.at[pl.ds(0, 15 * SLOTS)]
    pltpu.make_async_copy(most, most, send).wait()
    pltpu.make_async_copy(cot_out, cot_out, crecv).wait()
    most = cot_out.at[pl.ds(0, 127 * SLOTS)]
    pltpu.make_async_copy(most, most, csend).wait()


def body(tokens_in, cotangents, left_root, right_root):
    rows, width = tokens_in.shape
    columns = cotangents.shape[1] // lax.axis_size("replica")
    tokens, routed = pl.pallas_call(
        exchange,
        out_shape=(
            jax.ShapeDtypeStruct((rows, width), jnp.bfloat16),
            jax.ShapeDtypeStruct((rows * 8, columns), jnp.bfloat16),
        ),
        in_specs=[pl.BlockSpec(memory_space=pl.ANY)] * 2,
        out_specs=[pl.BlockSpec(memory_space=pltpu.VMEM)] * 2,
        scratch_shapes=[pltpu.SemaphoreType.DMA] * 4 + [pltpu.SemaphoreType.REGULAR] * 2,
        compiler_params=pltpu.CompilerParams(collective_id=0, has_side_effects=True),
    )(tokens_in, cotangents)
    left = lax.dot_general(
        left_root[0], tokens, (((1,), (1,)), ((), ())), preferred_element_type=jnp.float32
    ).astype(jnp.bfloat16)
    gathered = lax.all_gather(left, "replica", axis=0, tiled=False)
    right = jnp.dot(routed, right_root[0, 0], preferred_element_type=jnp.float32).astype(jnp.bfloat16)
    right = right.reshape(8, rows, columns)
    update = jnp.einsum("qdt,qtf->df", gathered, right, preferred_element_type=jnp.float32)
    return update.astype(jnp.bfloat16)[None]


def solution(mesh):
    placed = (
        P(BOTH, None),
        P(BOTH, None),
        P("expert", None, None),
        P("expert", "replica", None, None),
    )
    return jax.shard_map(
        body, mesh=mesh, in_specs=placed, out_specs=P("expert", None, "replica"), check_vma=False
    )
```

```python
import functools

import jax
import jax.numpy as jnp
from jax import lax
from jax.experimental import pallas as pl
from jax.experimental.pallas import tpu as pltpu
from jax.sharding import PartitionSpec as P

MESH = pl.DeviceIdType.MESH
SLOTS = 16
BOTH = ("expert", "replica")
TILE = 256
FIRST = 1152
STEPS = ((2, 0), (2, 1), (1, 0), (1, 1), (3, 0), (3, 1), (0, 0), (0, 1))
EARLY = 3


def position():
    e, r = lax.axis_index("expert"), lax.axis_index("replica")
    return ((e // 2) % 2) * 2 + r % 2, e // 4, r // 2, e % 2


def device(x, y, z, c):
    return (y * 2 + x // 2) * 2 + c, z * 2 + x % 2


def near(x, half):
    other = (x // 2 - half) * (x // 2 - half)
    return x + other * (3 - 2 * x)


def signal(semaphore, to):
    pl.semaphore_signal(semaphore, inc=1, device_id=to, device_id_type=MESH)


def drain(ref, semaphore):
    pltpu.make_async_copy(ref, ref, semaphore).wait()


def kernel(
    tok, cot, left_hbm, right_hbm, out,
    left, right, tokens, routed, lefts, rights, total,
    load, tok_send, tok_recv, cot_send, cot_recv, send, recv, plane_sem, all_sem,
):
    x, y, z, c = position()
    e, r = lax.axis_index("expert"), lax.axis_index("replica")
    columns = rights.shape[2]
    rows = tokens.shape[0]
    depth = left.shape[0]
    place = ((y * 2 + c) * 2 + x // 2) * SLOTS
    beside = x + 1 - 2 * (x % 2)
    bx = beside % 2
    mx = x % 2
    above, below = (z + 1) % 4, (z + 3) % 4

    load_left = pltpu.make_async_copy(left_hbm, left, load.at[0])
    load_right = pltpu.make_async_copy(right_hbm, right, load.at[1])
    load_left.start()
    load_right.start()

    barrier = pltpu.get_barrier_semaphore()

    def token_peer(k):
        half, up, core = k % 2, (k // 2) % 4, k // 8
        return device(x + half * (3 - 2 * x), (y + up) % 4, z, (c + core) % 2)

    def greet(k, _):
        signal(barrier, token_peer(k))
        return 0

    lax.fori_loop(1, 16, greet, 0)
    for up in (1, 2, 3):
        signal(barrier, device(x, y, (z + up) % 4, c))
    signal(barrier, device(beside, y, z, c))
    pl.semaphore_wait(barrier, 19)
    for up in (1, 2, 3):
        signal(plane_sem, device(x, y, (z + up) % 4, c))

    def send_tokens(k, _):
        to = token_peer(k)
        pltpu.make_async_remote_copy(
            tok.at[pl.ds(to[0] * SLOTS, SLOTS)], tokens.at[pl.ds(place, SLOTS)],
            tok_send, tok_recv, device_id=to, device_id_type=MESH,
        ).start()
        return 0

    lax.fori_loop(1, 16, send_tokens, 0)
    pltpu.make_async_copy(tok.at[pl.ds(e * SLOTS, SLOTS)], tokens.at[pl.ds(place, SLOTS)], tok_recv).start()
    pl.semaphore_wait(plane_sem, 3)
    signal(all_sem, device(beside, y, z, c))
    pl.semaphore_wait(all_sem, 1)

    def chunk_of(half):
        return z * 2 + near(x, half) % 2

    pltpu.make_async_copy(
        cot.at[pl.ds(e * SLOTS, SLOTS), pl.ds(r * columns, columns)],
        routed.at[chunk_of(x // 2), pl.ds(place, SLOTS)], cot_recv.at[chunk_of(x // 2)],
    ).start()

    def send_cotangents(step):
        lift, core = STEPS[step]

        def one(k, _):
            a, b = k % 4, k // 4
            tx = (x + a) % 4
            to = device(tx, (y + a + b) % 4, (z + a + lift) % 4, (c + core) % 2)
            chunk = chunk_of(tx // 2)
            pltpu.make_async_remote_copy(
                cot.at[pl.ds(to[0] * SLOTS, SLOTS), pl.ds(to[1] * columns, columns)],
                routed.at[chunk, pl.ds(place, SLOTS)],
                cot_send.at[step], cot_recv.at[chunk], device_id=to, device_id_type=MESH,
            ).start()
            return 0

        lax.fori_loop(1 if STEPS[step] == (0, 0) else 0, 16, one, 0)

    def sent_cotangents(step):
        size = 15 if STEPS[step] == (0, 0) else 16
        drain(routed.at[0, pl.ds(0, size * SLOTS)], cot_send.at[step])

    parts = {"a": (0, FIRST), "b": (FIRST, depth - FIRST)}
    half = (depth - FIRST) // 2
    if half:
        parts["c"] = (FIRST, half)
        parts["d"] = (FIRST + half, half)
    names = [(s, dz, p) for s in (0, 1) for dz in (0, 1, 2, 3) for p in "abcd"]
    flight = []

    def block(s, dz, part):
        start, size = parts[part]
        return lefts.at[((z + dz) % 4) * 2 + (bx if s else mx), pl.ds(start, size)]

    def push(s, dz, part, to):
        if parts[part][1] == 0:
            return
        if to == "beside":
            there, name = device(beside, y, z, c), (1 - s, dz, part)
        elif to == "above":
            there, name = device(x, y, above, c), (s, (dz + 3) % 4, part)
        else:
            there, name = device(x, y, below, c), (s, (dz + 1) % 4, part)
        ref = block(s, dz, part)
        copy = pltpu.make_async_remote_copy(
            ref, ref, send.at[len(flight)], recv.at[names.index(name)],
            device_id=there, device_id_type=MESH,
        )
        copy.start()
        flight.append((ref, send.at[len(flight)]))

    def arrived(s, dz, part):
        if parts[part][1]:
            drain(block(s, dz, part), recv.at[names.index((s, dz, part))])

    def apply_left(start, size):
        @pl.loop(0, size, step=TILE // 2)
        def _(row):
            at = pl.ds(start + row, TILE // 2)
            lefts[r, at] = lax.dot_general(
                left[at], tokens[...], (((1,), (1,)), ((), ())), preferred_element_type=jnp.float32
            ).astype(jnp.bfloat16)

    def apply_right(chunk):
        drain(routed.at[chunk], cot_recv.at[chunk])
        rights[chunk] = jnp.dot(
            routed[chunk], right[...], preferred_element_type=jnp.float32
        ).astype(jnp.bfloat16)

    def accumulate(chunks, part, first=False, last=False):
        start, size = parts[part]

        @pl.loop(0, size, step=TILE // 2)
        def _(row):
            at = pl.ds(start + row, TILE // 2)
            value = None if first else total[at]
            for chunk in chunks:
                term = jnp.dot(lefts[chunk, at], rights[chunk], preferred_element_type=jnp.float32)
                value = term if value is None else value + term
            if last:
                out[at] = value.astype(out.dtype)
            else:
                total[at] = value

    def chunk(s, dz):
        return ((z + dz) % 4) * 2 + (bx if s else mx)

    for step in range(EARLY):
        send_cotangents(step)
    drain(tokens, tok_recv)
    load_left.wait()
    apply_left(*parts["a"])
    if half:
        apply_left(*parts["b"])
    push(0, 0, "a", "beside")
    push(0, 0, "b", "above")
    push(0, 0, "b", "below")
    push(0, 0, "a", "above")
    push(0, 0, "a", "below")
    push(0, 0, "b", "beside")
    for step in range(EARLY, 8):
        sent_cotangents(step - EARLY)
        send_cotangents(step)
        if step == EARLY + 1:
            arrived(1, 0, "a")
            push(1, 0, "a", "above")
            push(1, 0, "a", "below")
    if half:
        arrived(0, 3, "b")
        push(0, 3, "c", "above")
        push(0, 3, "b", "beside")
        arrived(0, 1, "b")
        push(0, 1, "d", "below")
        push(0, 1, "b", "beside")
    arrived(0, 3, "a")
    push(0, 3, "a", "above")
    arrived(1, 1, "a")
    push(1, 1, "a", "below")
    if half:
        arrived(0, 2, "c")
        push(0, 2, "c", "beside")
        arrived(0, 2, "d")
        push(0, 2, "d", "beside")
    load_right.wait()
    for s in (0, 1):
        for dz in (0, 1, 3, 2):
            apply_right(chunk(s, dz))
    both = lambda dz: [chunk(0, dz), chunk(1, dz)]
    if half:
        arrived(1, 0, "b")
    accumulate(both(0), "a", first=True)
    accumulate(both(0), "b", first=True)
    arrived(1, 3, "a")
    arrived(0, 1, "a")
    if half:
        arrived(1, 1, "b")
        arrived(1, 3, "b")
    for part in "ab":
        accumulate(both(1) + both(3), part)
    arrived(0, 2, "a")
    arrived(1, 2, "a")
    accumulate(both(2), "a", last=True)
    if half:
        arrived(1, 2, "c")
        arrived(1, 2, "d")
        accumulate(both(2), "b", last=True)

    drain(tokens.at[pl.ds(0, 15 * SLOTS)], tok_send)
    for step in range(8 - EARLY, 8):
        sent_cotangents(step)
    for ref, semaphore in flight:
        drain(ref, semaphore)


def body(tokens_in, cotangents, left_root, right_root):
    rows, depth = tokens_in.shape
    columns = right_root.shape[3]
    bf16 = jnp.bfloat16
    update = pl.pallas_call(
        kernel,
        out_shape=jax.ShapeDtypeStruct((depth, columns), bf16),
        in_specs=[pl.BlockSpec(memory_space=pl.ANY)] * 4,
        out_specs=pl.BlockSpec(memory_space=pltpu.VMEM),
        scratch_shapes=[
            pltpu.VMEM((depth, depth), bf16),
            pltpu.VMEM((columns, columns), bf16),
            pltpu.VMEM((rows, depth), bf16),
            pltpu.VMEM((8, rows, columns), bf16),
            pltpu.VMEM((8, depth, rows), bf16),
            pltpu.VMEM((8, rows, columns), bf16),
            pltpu.VMEM((depth, columns), jnp.float32),
            pltpu.SemaphoreType.DMA((2,)),
            pltpu.SemaphoreType.DMA,
            pltpu.SemaphoreType.DMA,
            pltpu.SemaphoreType.DMA((8,)),
            pltpu.SemaphoreType.DMA((8,)),
            pltpu.SemaphoreType.DMA((24,)),
            pltpu.SemaphoreType.DMA((32,)),
            pltpu.SemaphoreType.REGULAR,
            pltpu.SemaphoreType.REGULAR,
        ],
        compiler_params=pltpu.CompilerParams(
            collective_id=0, has_side_effects=True, vmem_limit_bytes=60 << 20
        ),
    )(tokens_in, cotangents, left_root[0], right_root[0, 0])
    return update[None]


def solution(mesh):
    placed = (
        P(BOTH, None),
        P(BOTH, None),
        P("expert", None, None),
        P("expert", "replica", None, None),
    )
    return jax.shard_map(
        body, mesh=mesh, in_specs=placed, out_specs=P("expert", None, "replica"), check_vma=False
    )
```

```python
import functools

import jax
import jax.numpy as jnp
from jax import lax
from jax.experimental import pallas as pl
from jax.experimental.pallas import tpu as pltpu
from jax.sharding import PartitionSpec as P

MESH = pl.DeviceIdType.MESH
SLOTS = 16
BOTH = ("expert", "replica")
GROUPS = ((352, 272), (320, 256), (272, 208), (208, 160))
PIECES = len(GROUPS)
ROUTED = ()
OWN = ((0, 1), (2,), (3,), (), (), (), ())
STEPS = ((2, 0), (2, 1), (1, 0), (1, 1), (3, 0), (3, 1), (0, 0), (0, 1))
PLAN = ((1, 2, 3, 4), (5, 6, 7), (), (), (), (), ())
LAG = 6
RIGHTS = (0, 0, 0, 4, 0, 0, 0)
FINISH = ((), (), (), (0,), (1,), (2,), ())


def pieces():
    spans, start = {}, 0
    for i, (first, second) in enumerate(GROUPS):
        spans["a", i] = (start, first)
        spans["b", i] = (start + first, second)
        spans[i] = (start, first + second)
        start += first + second
    return spans


def product(lefts, rights, at, out):
    @pl.loop(0, rights.shape[2], step=256)
    def _(column):
        to = pl.ds(pl.multiple_of(column, 256), 256)
        value = None
        for q in range(8):
            term = jnp.dot(lefts[q, at], rights[q, :, to], preferred_element_type=jnp.float32)
            value = term if value is None else value + term
        out[:, to] = value.astype(out.dtype)


def position():
    e, r = lax.axis_index("expert"), lax.axis_index("replica")
    return ((e // 2) % 2) * 2 + r % 2, e // 4, r // 2, e % 2


def device(x, y, z, c):
    return (y * 2 + x // 2) * 2 + c, z * 2 + x % 2


def near(x, half):
    other = (x // 2 - half) * (x // 2 - half)
    return x + other * (3 - 2 * x)


def signal(semaphore, to):
    pl.semaphore_signal(semaphore, inc=1, device_id=to, device_id_type=MESH)


def drain(ref, semaphore):
    pltpu.make_async_copy(ref, ref, semaphore).wait()


def kernel(
    tok, cot, left_hbm, right_hbm, out, lefts, rights,
    left, right, tokens, routed,
    load, tok_send, tok_recv, cot_send, cot_recv, send, recv, plane_sem, all_sem,
):
    x, y, z, c = position()
    e, r = lax.axis_index("expert"), lax.axis_index("replica")
    columns = rights.shape[2]
    depth = left.shape[0]
    place = ((y * 2 + c) * 2 + x // 2) * SLOTS
    beside = x + 1 - 2 * (x % 2)

    load_left = pltpu.make_async_copy(left_hbm, left, load.at[0])
    load_right = pltpu.make_async_copy(right_hbm, right, load.at[1])
    load_left.start()
    load_right.start()

    barrier = pltpu.get_barrier_semaphore()

    def token_peer(k):
        half, up, core = k % 2, (k // 2) % 4, k // 8
        return device(x + half * (3 - 2 * x), (y + up) % 4, z, (c + core) % 2)

    def greet(k, _):
        signal(barrier, token_peer(k))
        return 0

    lax.fori_loop(1, 16, greet, 0)
    for up in (1, 2, 3):
        signal(barrier, device(x, y, (z + up) % 4, c))
    signal(barrier, device(beside, y, z, c))
    pl.semaphore_wait(barrier, 19)
    for up in (1, 2, 3):
        signal(plane_sem, device(x, y, (z + up) % 4, c))

    def send_tokens(k, _):
        to = token_peer(k)
        pltpu.make_async_remote_copy(
            tok.at[pl.ds(to[0] * SLOTS, SLOTS)], tokens.at[pl.ds(place, SLOTS)],
            tok_send, tok_recv, device_id=to, device_id_type=MESH,
        ).start()
        return 0

    lax.fori_loop(1, 16, send_tokens, 0)
    pltpu.make_async_copy(tok.at[pl.ds(e * SLOTS, SLOTS)], tokens.at[pl.ds(place, SLOTS)], tok_recv).start()
    pl.semaphore_wait(plane_sem, 3)
    signal(all_sem, device(beside, y, z, c))
    pl.semaphore_wait(all_sem, 1)

    def chunk_of(half):
        return z * 2 + near(x, half) % 2

    pltpu.make_async_copy(
        cot.at[pl.ds(e * SLOTS, SLOTS), pl.ds(r * columns, columns)],
        routed.at[chunk_of(x // 2), pl.ds(place, SLOTS)], cot_recv.at[chunk_of(x // 2)],
    ).start()

    def send_one(step, turn, up, lift, core):
        over = turn // 2
        side = ((turn + 1) // 2) % 2
        high, low = x // 2 + over - 2 * over * (x // 2), x % 2 + side - 2 * side * (x % 2)
        to = device(high * 2 + low, (y + up) % 4, (z + lift) % 4, (c + core) % 2)
        chunk = chunk_of(high)
        pltpu.make_async_remote_copy(
            cot.at[pl.ds(to[0] * SLOTS, SLOTS), pl.ds(to[1] * columns, columns)],
            routed.at[chunk, pl.ds(place, SLOTS)],
            cot_send.at[step], cot_recv.at[chunk], device_id=to, device_id_type=MESH,
        ).start()

    def send_near():
        def one(k, _):
            send_one(8, k % 2, 0, (k // 2) % 4, k // 8)
            return 0

        lax.fori_loop(1, 16, one, 0)

    def send_far(step):
        lift, core = STEPS[step]

        def one(k, _):
            a, b = k % 4, k // 4
            send_one(step, a, (a + b) % 4, (a + lift) % 4, core)
            return 0

        lax.fori_loop(1, 13, one, 0)
        lax.fori_loop(14, 16, one, 0)

    def sent(step):
        drain(routed.at[0, pl.ds(0, (15 if step == 8 else 14) * SLOTS)], cot_send.at[step])

    parts = pieces()
    names = [(s, dz, (p, i)) for s in (0, 1) for dz in (0, 1, 2, 3) for p in "ab" for i in range(PIECES)]
    flight = {}

    def chunk(s, dz):
        return ((z + dz) % 4) * 2 + (beside if s else x) % 2

    def block(s, dz, part):
        return lefts.at[chunk(s, dz), pl.ds(*parts[part])]

    def push(s, dz, part, to):
        if to == "beside":
            there, name = device(beside, y, z, c), (1 - s, dz, part)
        elif to == "above":
            there, name = device(x, y, (z + 1) % 4, c), (s, (dz + 3) % 4, part)
        elif to == "below":
            there, name = device(x, y, (z + 3) % 4, c), (s, (dz + 1) % 4, part)
        else:
            there, name = device(x, y, (z + 2) % 4, c), (s, (dz + 2) % 4, part)
        ref = block(s, dz, part)
        kind = (s, dz > 0, part[0] == "a", to == "beside")
        rows = flight.setdefault(kind, [])
        rows.append(parts[part][1])
        pltpu.make_async_remote_copy(
            ref, ref, send.at[list(flight).index(kind)], recv.at[names.index(name)],
            device_id=there, device_id_type=MESH,
        ).start()

    def arrived(s, dz, part):
        drain(block(s, dz, part), recv.at[names.index((s, dz, part))])

    def apply_left(part):
        at = pl.ds(*parts[part])
        lefts[r, at] = lax.dot_general(
            left[at], tokens[...], (((1,), (1,)), ((), ())), preferred_element_type=jnp.float32
        ).astype(jnp.bfloat16)

    def apply_right(dz):
        at = pl.ds(((z + dz) % 4) * 2, 2)
        for s in (0, 1):
            drain(routed.at[chunk(s, dz)], cot_recv.at[chunk(s, dz)])
        both = routed[at].reshape(512, columns)
        rights[at] = jnp.dot(both, right[...], preferred_element_type=jnp.float32).astype(
            jnp.bfloat16
        ).reshape(2, 256, columns)

    def multiply(part):
        at = pl.ds(*parts[part])
        product(lefts, rights, at, out.at[at])

    def push_own(part):
        for to in ("beside", "above", "below") if part[0] == "a" else ("above", "below", "beside"):
            push(0, 0, part, to)
        if part[1] in ROUTED:
            push(0, 0, part, "over")

    waited = []

    def far(steps):
        for step in steps:
            old = 8 if step == LAG - 1 else step - LAG
            if old >= 0:
                sent(old)
                waited.append(old)
            send_far(step)

    turns = [0, 1, 3, 2]

    def some_right(count):
        for _ in range(count):
            if len(turns) == 4:
                load_right.wait()
            apply_right(turns.pop(0))

    def arrivals(i):
        part = ("a", i)
        late = ((0, 3), (1, 1)) if i in ROUTED else ()
        for s, dz in late + ((1, 3), (0, 1), (0, 2), (1, 2)):
            arrived(s, dz, part)
        part = ("b", i)
        for dz in (0, 1, 3, 2):
            arrived(1, dz, part)

    def push_group(i):
        push_own(("a", i))
        push_own(("b", i))

    ready = [0]

    def prepare(upto):
        while ready[0] < min(upto, PIECES):
            apply_left(ready[0])
            ready[0] += 1

    send_near()
    drain(tokens.at[pl.ds(0, 15 * SLOTS)], tok_send)
    send_far(0)
    load_left.wait()
    drain(tokens, tok_recv)
    prepare(1)
    for step in range(PIECES + 3):
        last, older = (i if 0 <= i < PIECES else None for i in (step - 1, step - 2))
        if older is not None and older not in ROUTED:
            arrived(0, 3, ("a", older))
            push(0, 3, ("a", older), "above")
            arrived(1, 1, ("a", older))
            push(1, 1, ("a", older), "below")
        if last is not None:
            part = ("a", last)
            arrived(1, 0, part)
            push(1, 0, part, "above")
            push(1, 0, part, "below")
            if last in ROUTED:
                push(1, 0, part, "over")
            part = ("b", last)
            arrived(0, 3, part)
            arrived(0, 1, part)
            if last not in ROUTED:
                if last % 2:
                    push(0, 1, part, "below")
                else:
                    push(0, 3, part, "above")
            push(0, 1, part, "beside")
            push(0, 3, part, "beside")
            if last in ROUTED:
                arrived(0, 2, part)
                push(0, 2, part, "beside")
        for own in OWN[step]:
            prepare(own + 2)
            push_group(own)
        far(PLAN[step])
        if older is not None and older not in ROUTED:
            part = ("b", older)
            arrived(0, 2, part)
            push(0, 2, part, "beside")
        some_right(RIGHTS[step])
        for i in FINISH[step]:
            arrivals(i)
            multiply(i)
    arrivals(PIECES - 1)

    for step in range(9):
        if step not in waited:
            sent(step)
    for i, rows in enumerate(flight.values()):
        times = next(n for n in (1, 2, 3, 4, 5, 6, 7, 8) if sum(rows) % n == 0 and sum(rows) // n <= depth)
        drain(lefts.at[pl.ds(0, times), pl.ds(0, sum(rows) // times)], send.at[i])


def ending(done, lefts, rights, out, rest, sems):
    start, size = pieces()[PIECES - 1]
    whole = pltpu.make_async_copy(done.at[pl.ds(0, start)], out.at[pl.ds(0, start)], sems.at[0])
    whole.start()
    product(lefts, rights, pl.ds(start, size), rest)
    last = pltpu.make_async_copy(rest, out.at[pl.ds(start, size)], sems.at[1])
    last.start()
    whole.wait()
    last.wait()


def body(tokens_in, cotangents, left_root, right_root):
    rows, depth = tokens_in.shape
    columns = right_root.shape[3]
    bf16 = jnp.bfloat16
    vmem, anywhere = pl.BlockSpec(memory_space=pltpu.VMEM), pl.BlockSpec(memory_space=pl.ANY)
    done, lefts, rights = pl.pallas_call(
        kernel,
        out_shape=(
            pltpu.VMEM((depth, columns), bf16),
            pltpu.VMEM((8, depth, rows), bf16),
            pltpu.VMEM((8, rows, columns), bf16),
        ),
        in_specs=[anywhere] * 4,
        out_specs=(vmem,) * 3,
        scratch_shapes=[
            pltpu.VMEM((depth, depth), bf16),
            pltpu.VMEM((columns, columns), bf16),
            pltpu.VMEM((rows, depth), bf16),
            pltpu.VMEM((8, rows, columns), bf16),
            pltpu.SemaphoreType.DMA((2,)),
            pltpu.SemaphoreType.DMA,
            pltpu.SemaphoreType.DMA,
            pltpu.SemaphoreType.DMA((9,)),
            pltpu.SemaphoreType.DMA((8,)),
            pltpu.SemaphoreType.DMA((16,)),
            pltpu.SemaphoreType.DMA((16 * PIECES,)),
            pltpu.SemaphoreType.REGULAR,
            pltpu.SemaphoreType.REGULAR,
        ],
        compiler_params=pltpu.CompilerParams(
            collective_id=0, has_side_effects=True, vmem_limit_bytes=40 << 20
        ),
    )(tokens_in, cotangents, left_root[0], right_root[0, 0])
    update = pl.pallas_call(
        ending,
        out_shape=jax.ShapeDtypeStruct((depth, columns), bf16),
        in_specs=[vmem] * 3,
        out_specs=anywhere,
        scratch_shapes=[
            pltpu.VMEM((sum(GROUPS[-1]), columns), bf16),
            pltpu.SemaphoreType.DMA((2,)),
        ],
        compiler_params=pltpu.CompilerParams(vmem_limit_bytes=20 << 20),
    )(done, lefts, rights)
    return update[None]


def solution(mesh):
    placed = (
        P(BOTH, None),
        P(BOTH, None),
        P("expert", None, None),
        P("expert", "replica", None, None),
    )
    return jax.shard_map(
        body, mesh=mesh, in_specs=placed, out_specs=P("expert", None, "replica"), check_vma=False
    )
```

```python
import functools

import jax
import jax.numpy as jnp
from jax import lax
from jax.experimental import pallas as pl
from jax.experimental.pallas import tpu as pltpu
from jax.sharding import PartitionSpec as P

MESH = pl.DeviceIdType.MESH
SLOTS = 16
BOTH = ("expert", "replica")
GROUPS = ((320, 320), (288, 288), (240, 240), (176, 176))
PIECES = len(GROUPS)
STEPS = ((2, 0), (2, 1), (1, 0), (1, 1), (3, 0), (3, 1), (0, 0), (0, 1))
PLAN = ((2, 3, 4), (5, 6), (7,), ())
LAG = 6
RIGHTS = (0, 4, 0, 0)
SUMS = ((), (0,), (1,), (2,))


def pieces():
    spans, start = {}, 0
    for i, (first, second) in enumerate(GROUPS):
        spans["a", i] = (start, first)
        spans["b", i] = (start + first, second)
        spans[i] = (start, first + second)
        start += first + second
    return spans


def product(lefts, rights, chunks, at, out, total=None, into=None):
    @pl.loop(0, rights.shape[2], step=256)
    def _(column):
        to = pl.ds(pl.multiple_of(column, 256), 256)
        value = None if total is None else total[at if into is None else into, to]
        for q in chunks:
            term = jnp.dot(lefts[q, at], rights[q, :, to], preferred_element_type=jnp.float32)
            value = term if value is None else value + term
        out[at if into is None else into, to] = value.astype(out.dtype)


def position():
    e, r = lax.axis_index("expert"), lax.axis_index("replica")
    return ((e // 2) % 2) * 2 + r % 2, e // 4, r // 2, e % 2


def device(x, y, z, c):
    return (y * 2 + x // 2) * 2 + c, z * 2 + x % 2


def near(x, half):
    other = (x // 2 - half) * (x // 2 - half)
    return x + other * (3 - 2 * x)


def signal(semaphore, to):
    pl.semaphore_signal(semaphore, inc=1, device_id=to, device_id_type=MESH)


def drain(ref, semaphore):
    pltpu.make_async_copy(ref, ref, semaphore).wait()


def kernel(
    tok, cot, left_hbm, right_hbm, out, lefts, rights, total_last,
    left, right, tokens, routed, total,
    load, tok_send, tok_recv, cot_send, cot_recv, send, recv, plane_sem, all_sem,
):
    x, y, z, c = position()
    e, r = lax.axis_index("expert"), lax.axis_index("replica")
    columns = rights.shape[2]
    depth = left.shape[0]
    place = ((y * 2 + c) * 2 + x // 2) * SLOTS
    beside = x + 1 - 2 * (x % 2)

    load_left = pltpu.make_async_copy(left_hbm, left, load.at[0])
    load_right = pltpu.make_async_copy(right_hbm, right, load.at[1])
    load_left.start()
    load_right.start()

    barrier = pltpu.get_barrier_semaphore()

    def token_peer(k):
        half, up, core = k % 2, (k // 2) % 4, k // 8
        return device(x + half * (3 - 2 * x), (y + up) % 4, z, (c + core) % 2)

    def greet(k, _):
        signal(barrier, token_peer(k))
        return 0

    lax.fori_loop(1, 16, greet, 0)
    for up in (1, 2, 3):
        signal(barrier, device(x, y, (z + up) % 4, c))
    signal(barrier, device(beside, y, z, c))
    pl.semaphore_wait(barrier, 19)
    for up in (1, 2, 3):
        signal(plane_sem, device(x, y, (z + up) % 4, c))

    def send_tokens(k, _):
        to = token_peer(k)
        pltpu.make_async_remote_copy(
            tok.at[pl.ds(to[0] * SLOTS, SLOTS)], tokens.at[pl.ds(place, SLOTS)],
            tok_send, tok_recv, device_id=to, device_id_type=MESH,
        ).start()
        return 0

    lax.fori_loop(1, 16, send_tokens, 0)
    pltpu.make_async_copy(tok.at[pl.ds(e * SLOTS, SLOTS)], tokens.at[pl.ds(place, SLOTS)], tok_recv).start()
    pl.semaphore_wait(plane_sem, 3)
    signal(all_sem, device(beside, y, z, c))
    pl.semaphore_wait(all_sem, 1)

    def chunk_of(half):
        return z * 2 + near(x, half) % 2

    pltpu.make_async_copy(
        cot.at[pl.ds(e * SLOTS, SLOTS), pl.ds(r * columns, columns)],
        routed.at[chunk_of(x // 2), pl.ds(place, SLOTS)], cot_recv.at[chunk_of(x // 2)],
    ).start()

    def send_one(step, turn, up, lift, core):
        over = turn // 2
        side = ((turn + 1) // 2) % 2
        high, low = x // 2 + over - 2 * over * (x // 2), x % 2 + side - 2 * side * (x % 2)
        to = device(high * 2 + low, (y + up) % 4, (z + lift) % 4, (c + core) % 2)
        chunk = chunk_of(high)
        pltpu.make_async_remote_copy(
            cot.at[pl.ds(to[0] * SLOTS, SLOTS), pl.ds(to[1] * columns, columns)],
            routed.at[chunk, pl.ds(place, SLOTS)],
            cot_send.at[step], cot_recv.at[chunk], device_id=to, device_id_type=MESH,
        ).start()

    def send_near():
        def one(k, _):
            send_one(8, k % 2, 0, (k // 2) % 4, k // 8)
            return 0

        lax.fori_loop(1, 16, one, 0)

    def send_far(step):
        lift, core = STEPS[step]

        def one(k, _):
            a, b = k % 4, k // 4
            send_one(step, a, (a + b) % 4, (a + lift) % 4, core)
            return 0

        lax.fori_loop(1, 13, one, 0)
        lax.fori_loop(14, 16, one, 0)

    def sent(step):
        drain(routed.at[0, pl.ds(0, (15 if step == 8 else 14) * SLOTS)], cot_send.at[step])

    parts = pieces()
    names = [(s, dz, (p, i)) for s in (0, 1) for dz in (0, 1, 2, 3) for p in "ab" for i in range(PIECES)]
    flight = {}

    def chunk(s, dz):
        return ((z + dz) % 4) * 2 + (beside if s else x) % 2

    def block(s, dz, part):
        return lefts.at[chunk(s, dz), pl.ds(*parts[part])]

    def push(s, dz, part, to):
        if to == "beside":
            there, name = device(beside, y, z, c), (1 - s, dz, part)
        elif to == "above":
            there, name = device(x, y, (z + 1) % 4, c), (s, (dz + 3) % 4, part)
        else:
            there, name = device(x, y, (z + 3) % 4, c), (s, (dz + 1) % 4, part)
        ref = block(s, dz, part)
        kind = (s, dz > 0, part[0] == "a", to == "beside")
        rows = flight.setdefault(kind, [])
        rows.append(parts[part][1])
        pltpu.make_async_remote_copy(
            ref, ref, send.at[list(flight).index(kind)], recv.at[names.index(name)],
            device_id=there, device_id_type=MESH,
        ).start()

    def arrived(s, dz, part):
        drain(block(s, dz, part), recv.at[names.index((s, dz, part))])

    def apply_left(part):
        at = pl.ds(*parts[part])
        lefts[r, at] = lax.dot_general(
            left[at], tokens[...], (((1,), (1,)), ((), ())), preferred_element_type=jnp.float32
        ).astype(jnp.bfloat16)

    def apply_right(dz):
        at = pl.ds(((z + dz) % 4) * 2, 2)
        for s in (0, 1):
            drain(routed.at[chunk(s, dz)], cot_recv.at[chunk(s, dz)])
        both = routed[at].reshape(512, columns)
        rights[at] = jnp.dot(both, right[...], preferred_element_type=jnp.float32).astype(
            jnp.bfloat16
        ).reshape(2, 256, columns)

    def first_sum(i):
        for s, dz in ((1, 3), (0, 1)):
            arrived(s, dz, ("a", i))
        for dz in (0, 1, 3):
            arrived(1, dz, ("b", i))
        first = [chunk(s, dz) for dz in (0, 1, 3) for s in (0, 1)]
        at = pl.ds(*parts[i])
        if i + 1 < PIECES:
            product(lefts, rights, first, at, total)
        else:
            product(lefts, rights, first, at, total_last, into=pl.ds(0, at.size))

    def second_sum(i):
        for s in (0, 1):
            arrived(s, 2, ("a", i))
        arrived(1, 2, ("b", i))
        if i + 1 < PIECES:
            product(lefts, rights, [chunk(0, 2), chunk(1, 2)], pl.ds(*parts[i]), out, total)

    def push_own(part):
        for to in ("beside", "above", "below") if part[0] == "a" else ("above", "below", "beside"):
            push(0, 0, part, to)

    waited = []

    def far(steps):
        for step in steps:
            old = 8 if step == LAG - 1 else step - LAG
            if old >= 0:
                sent(old)
                waited.append(old)
            send_far(step)

    turns = [0, 1, 3, 2]

    def some_right(count):
        for _ in range(count):
            if len(turns) == 4:
                load_right.wait()
            apply_right(turns.pop(0))

    def push_group(i):
        push_own(("a", i))
        push_own(("b", i))

    send_near()
    drain(tokens.at[pl.ds(0, 15 * SLOTS)], tok_send)
    send_far(0)
    load_left.wait()
    drain(tokens, tok_recv)
    for i in range(PIECES):
        apply_left(i)
        if i:
            push_group(i - 1)
    send_far(1)
    push_group(PIECES - 1)
    for i in range(PIECES):
        part = ("a", i)
        arrived(1, 0, part)
        push(1, 0, part, "above")
        push(1, 0, part, "below")
        far(PLAN[i])
        part = ("b", i)
        arrived(0, 3, part)
        arrived(0, 1, part)
        if i % 2:
            push(0, 1, part, "below")
        else:
            push(0, 3, part, "above")
        push(0, 1, part, "beside")
        push(0, 3, part, "beside")
    for i in range(PIECES):
        part = ("a", i)
        arrived(0, 3, part)
        push(0, 3, part, "above")
        arrived(1, 1, part)
        push(1, 1, part, "below")
        some_right(RIGHTS[i])
        part = ("b", i)
        arrived(0, 2, part)
        push(0, 2, part, "beside")
        for j in SUMS[i]:
            first_sum(j)
    first_sum(PIECES - 1)
    for i in range(PIECES):
        second_sum(i)

    for step in range(9):
        if step not in waited:
            sent(step)
    for i, rows in enumerate(flight.values()):
        times = next(n for n in (1, 2, 3, 4, 5, 6, 7, 8) if sum(rows) % n == 0 and sum(rows) // n <= depth)
        drain(lefts.at[pl.ds(0, times), pl.ds(0, sum(rows) // times)], send.at[i])


def ending(done, lefts, rights, total, out, rest, sems):
    start, size = pieces()[PIECES - 1]
    whole = pltpu.make_async_copy(done.at[pl.ds(0, start)], out.at[pl.ds(0, start)], sems.at[0])
    whole.start()
    at = pl.ds(start, size)
    z = lax.axis_index("replica") // 2
    far = ((z + 2) % 4) * 2
    product(lefts, rights, (far, far + 1), at, rest, total, into=pl.ds(0, size))
    last = pltpu.make_async_copy(rest, out.at[at], sems.at[1])
    last.start()
    whole.wait()
    last.wait()


def body(tokens_in, cotangents, left_root, right_root):
    rows, depth = tokens_in.shape
    columns = right_root.shape[3]
    bf16 = jnp.bfloat16
    vmem, anywhere = pl.BlockSpec(memory_space=pltpu.VMEM), pl.BlockSpec(memory_space=pl.ANY)
    done, lefts, rights, total = pl.pallas_call(
        kernel,
        out_shape=(
            pltpu.VMEM((depth, columns), bf16),
            pltpu.VMEM((8, depth, rows), bf16),
            pltpu.VMEM((8, rows, columns), bf16),
            pltpu.VMEM((sum(GROUPS[-1]), columns), jnp.float32),
        ),
        in_specs=[anywhere] * 4,
        out_specs=(vmem,) * 4,
        scratch_shapes=[
            pltpu.VMEM((depth, depth), bf16),
            pltpu.VMEM((columns, columns), bf16),
            pltpu.VMEM((rows, depth), bf16),
            pltpu.VMEM((8, rows, columns), bf16),
            pltpu.VMEM((depth - sum(GROUPS[-1]), columns), jnp.float32),
            pltpu.SemaphoreType.DMA((2,)),
            pltpu.SemaphoreType.DMA,
            pltpu.SemaphoreType.DMA,
            pltpu.SemaphoreType.DMA((9,)),
            pltpu.SemaphoreType.DMA((8,)),
            pltpu.SemaphoreType.DMA((16,)),
            pltpu.SemaphoreType.DMA((16 * PIECES,)),
            pltpu.SemaphoreType.REGULAR,
            pltpu.SemaphoreType.REGULAR,
        ],
        compiler_params=pltpu.CompilerParams(
            collective_id=0, has_side_effects=True, vmem_limit_bytes=40 << 20
        ),
    )(tokens_in, cotangents, left_root[0], right_root[0, 0])
    update = pl.pallas_call(
        ending,
        out_shape=jax.ShapeDtypeStruct((depth, columns), bf16),
        in_specs=[vmem] * 4,
        out_specs=anywhere,
        scratch_shapes=[
            pltpu.VMEM((sum(GROUPS[-1]), columns), bf16),
            pltpu.SemaphoreType.DMA((2,)),
        ],
        compiler_params=pltpu.CompilerParams(vmem_limit_bytes=20 << 20),
    )(done, lefts, rights, total)
    return update[None]


def solution(mesh):
    placed = (
        P(BOTH, None),
        P(BOTH, None),
        P("expert", None, None),
        P("expert", "replica", None, None),
    )
    return jax.shard_map(
        body, mesh=mesh, in_specs=placed, out_specs=P("expert", None, "replica"), check_vma=False
    )
```

```python
import functools

import jax
import jax.numpy as jnp
from jax import lax
from jax.experimental import pallas as pl
from jax.experimental.pallas import tpu as pltpu
from jax.sharding import PartitionSpec as P

MESH = pl.DeviceIdType.MESH
SLOTS = 16
BOTH = ("expert", "replica")
GROUPS = ((320, 320), (288, 288), (240, 240), (176, 176))
PIECES = len(GROUPS)
STEPS = ((0, 0, 0), (0, 0, 1), (0, 1, 0), (0, 1, 1), (1, 0, 0), (1, 0, 1), (1, 1, 0), (1, 1, 1))
PLAN = ((2, 3, 4), (5, 6), (7,), ())
LAG = 6
RIGHTS = (0, 0, 0, 2, 0, 2, 0, 0)
ZERO = ((), (), (), (0, 1, 2, 3), (), (), (), ())
SUMS = ((), (0,), (1,), (2,))


def pieces():
    spans, start = {}, 0
    for i, (first, second) in enumerate(GROUPS):
        spans["a", i] = (start, first)
        spans["b", i] = (start + first, second)
        spans[i] = (start, first + second)
        start += first + second
    return spans


def product(lefts, rights, chunks, at, out, total=None, into=None):
    @pl.loop(0, rights.shape[2], step=256)
    def _(column):
        to = pl.ds(pl.multiple_of(column, 256), 256)
        value = None if total is None else total[at if into is None else into, to]
        for q in chunks:
            term = jnp.dot(lefts[q, at], rights[q, :, to], preferred_element_type=jnp.float32)
            value = term if value is None else value + term
        out[at if into is None else into, to] = value.astype(out.dtype)


def position():
    e, r = lax.axis_index("expert"), lax.axis_index("replica")
    return ((e // 2) % 2) * 2 + r % 2, e // 4, r // 2, e % 2


def device(x, y, z, c):
    return (y * 2 + x // 2) * 2 + c, z * 2 + x % 2


def near(x, half):
    other = (x // 2 - half) * (x // 2 - half)
    return x + other * (3 - 2 * x)


def signal(semaphore, to):
    pl.semaphore_signal(semaphore, inc=1, device_id=to, device_id_type=MESH)


def drain(ref, semaphore):
    pltpu.make_async_copy(ref, ref, semaphore).wait()


def kernel(
    tok, cot, left_hbm, right_hbm, out, lefts, rights, total_last,
    left, right, tokens, routed, total,
    load, tok_send, tok_recv, cot_send, cot_recv, send, recv, plane_sem, all_sem,
):
    x, y, z, c = position()
    e, r = lax.axis_index("expert"), lax.axis_index("replica")
    columns = rights.shape[2]
    depth = left.shape[0]
    place = ((y * 2 + c) * 2 + x // 2) * SLOTS
    beside = x + 1 - 2 * (x % 2)

    load_left = pltpu.make_async_copy(left_hbm, left, load.at[0])
    load_right = pltpu.make_async_copy(right_hbm, right, load.at[1])
    load_left.start()
    load_right.start()

    barrier = pltpu.get_barrier_semaphore()

    def token_peer(k):
        half, up, core = k % 2, (k // 2) % 4, k // 8
        return device(x + half * (3 - 2 * x), (y + up) % 4, z, (c + core) % 2)

    def greet(k, _):
        signal(barrier, token_peer(k))
        return 0

    lax.fori_loop(1, 16, greet, 0)
    for up in (1, 2, 3):
        signal(barrier, device(x, y, (z + up) % 4, c))
    signal(barrier, device(beside, y, z, c))
    pl.semaphore_wait(barrier, 19)
    for up in (1, 2, 3):
        signal(plane_sem, device(x, y, (z + up) % 4, c))

    def send_tokens(k, _):
        to = token_peer(k)
        pltpu.make_async_remote_copy(
            tok.at[pl.ds(to[0] * SLOTS, SLOTS)], tokens.at[pl.ds(place, SLOTS)],
            tok_send, tok_recv, device_id=to, device_id_type=MESH,
        ).start()
        return 0

    lax.fori_loop(1, 16, send_tokens, 0)
    pltpu.make_async_copy(tok.at[pl.ds(e * SLOTS, SLOTS)], tokens.at[pl.ds(place, SLOTS)], tok_recv).start()
    pl.semaphore_wait(plane_sem, 3)
    signal(all_sem, device(beside, y, z, c))
    pl.semaphore_wait(all_sem, 1)

    def chunk_of(half):
        return z * 2 + near(x, half) % 2

    pltpu.make_async_copy(
        cot.at[pl.ds(e * SLOTS, SLOTS), pl.ds(r * columns, columns)],
        routed.at[chunk_of(x // 2), pl.ds(place, SLOTS)], cot_recv.at[chunk_of(x // 2)],
    ).start()

    def send_one(step, turn, up, lift, core):
        over = turn // 2
        side = ((turn + 1) // 2) % 2
        high, low = x // 2 + over - 2 * over * (x // 2), x % 2 + side - 2 * side * (x % 2)
        to = device(high * 2 + low, (y + up) % 4, (z + lift) % 4, (c + core) % 2)
        chunk = chunk_of(high)
        pltpu.make_async_remote_copy(
            cot.at[pl.ds(to[0] * SLOTS, SLOTS), pl.ds(to[1] * columns, columns)],
            routed.at[chunk, pl.ds(place, SLOTS)],
            cot_send.at[step], cot_recv.at[chunk], device_id=to, device_id_type=MESH,
        ).start()

    def send_near():
        def one(k, _):
            send_one(8, k % 2, 0, (k // 2) % 4, k // 8)
            return 0

        lax.fori_loop(1, 16, one, 0)

    def send_far(step):
        odd, turn, core = STEPS[step]

        def one(k, _):
            a, b = k % 4, k // 4
            send_one(step, a, (a + b) % 4, odd + 2 * ((a + turn) % 2), core)
            return 0

        lax.fori_loop(1, 13, one, 0)
        lax.fori_loop(14, 16, one, 0)

    def sent(step):
        drain(routed.at[0, pl.ds(0, (15 if step == 8 else 14) * SLOTS)], cot_send.at[step])

    parts = pieces()
    names = [(s, dz, (p, i)) for s in (0, 1) for dz in (0, 1, 2, 3) for p in "ab" for i in range(PIECES)]
    flight = {}

    def chunk(s, dz):
        return ((z + dz) % 4) * 2 + (beside if s else x) % 2

    def block(s, dz, part):
        return lefts.at[chunk(s, dz), pl.ds(*parts[part])]

    def push(s, dz, part, to):
        if to == "beside":
            there, name = device(beside, y, z, c), (1 - s, dz, part)
        elif to == "above":
            there, name = device(x, y, (z + 1) % 4, c), (s, (dz + 3) % 4, part)
        else:
            there, name = device(x, y, (z + 3) % 4, c), (s, (dz + 1) % 4, part)
        ref = block(s, dz, part)
        kind = (s, dz > 0, part[0] == "a", to == "beside")
        rows = flight.setdefault(kind, [])
        rows.append(parts[part][1])
        pltpu.make_async_remote_copy(
            ref, ref, send.at[list(flight).index(kind)], recv.at[names.index(name)],
            device_id=there, device_id_type=MESH,
        ).start()

    def arrived(s, dz, part):
        drain(block(s, dz, part), recv.at[names.index((s, dz, part))])

    def apply_left(part):
        at = pl.ds(*parts[part])
        lefts[r, at] = lax.dot_general(
            left[at], tokens[...], (((1,), (1,)), ((), ())), preferred_element_type=jnp.float32
        ).astype(jnp.bfloat16)

    def apply_right(dz):
        at = pl.ds(((z + dz) % 4) * 2, 2)
        for s in (0, 1):
            drain(routed.at[chunk(s, dz)], cot_recv.at[chunk(s, dz)])
        both = routed[at].reshape(512, columns)
        rights[at] = jnp.dot(both, right[...], preferred_element_type=jnp.float32).astype(
            jnp.bfloat16
        ).reshape(2, 256, columns)

    def add(i, chunks, begin=False):
        at = pl.ds(*parts[i])
        if i + 1 < PIECES:
            product(lefts, rights, chunks, at, total, None if begin else total)
        else:
            product(lefts, rights, chunks, at, total_last, None if begin else total_last, pl.ds(0, at.size))

    def zero_sum(i):
        arrived(1, 0, ("b", i))
        add(i, [chunk(0, 0), chunk(1, 0)], True)

    def first_sum(i):
        for s, dz in ((1, 3), (0, 1)):
            arrived(s, dz, ("a", i))
        for dz in (1, 3):
            arrived(1, dz, ("b", i))
        add(i, [chunk(s, dz) for dz in (1, 3) for s in (0, 1)])

    def second_sum(i):
        for s in (0, 1):
            arrived(s, 2, ("a", i))
        arrived(1, 2, ("b", i))
        if i + 1 < PIECES:
            product(lefts, rights, [chunk(0, 2), chunk(1, 2)], pl.ds(*parts[i]), out, total)

    def push_own(part):
        for to in ("beside", "above", "below") if part[0] == "a" else ("above", "below", "beside"):
            push(0, 0, part, to)

    waited = []

    def far(steps):
        for step in steps:
            old = 8 if step == LAG - 1 else step - LAG
            if old >= 0:
                sent(old)
                waited.append(old)
            send_far(step)

    turns = [0, 2, 1, 3]

    def some_right(count):
        for _ in range(count):
            if len(turns) == 4:
                load_right.wait()
            apply_right(turns.pop(0))

    def push_group(i):
        push_own(("a", i))
        push_own(("b", i))

    send_near()
    drain(tokens.at[pl.ds(0, 15 * SLOTS)], tok_send)
    send_far(0)
    load_left.wait()
    drain(tokens, tok_recv)
    for i in range(PIECES):
        apply_left(i)
        if i:
            push_group(i - 1)
    send_far(1)
    push_group(PIECES - 1)
    for i in range(PIECES):
        part = ("a", i)
        arrived(1, 0, part)
        push(1, 0, part, "above")
        push(1, 0, part, "below")
        far(PLAN[i])
        part = ("b", i)
        arrived(0, 3, part)
        arrived(0, 1, part)
        if i % 2:
            push(0, 1, part, "below")
        else:
            push(0, 3, part, "above")
        push(0, 1, part, "beside")
        push(0, 3, part, "beside")
        some_right(RIGHTS[i])
        for j in ZERO[i]:
            zero_sum(j)
    for i in range(PIECES):
        part = ("a", i)
        arrived(0, 3, part)
        push(0, 3, part, "above")
        arrived(1, 1, part)
        push(1, 1, part, "below")
        some_right(RIGHTS[PIECES + i])
        part = ("b", i)
        arrived(0, 2, part)
        push(0, 2, part, "beside")
        for j in ZERO[PIECES + i]:
            zero_sum(j)
        for j in SUMS[i]:
            first_sum(j)
    first_sum(PIECES - 1)
    for i in range(PIECES):
        second_sum(i)

    for step in range(9):
        if step not in waited:
            sent(step)
    for i, rows in enumerate(flight.values()):
        times = next(n for n in (1, 2, 3, 4, 5, 6, 7, 8) if sum(rows) % n == 0 and sum(rows) // n <= depth)
        drain(lefts.at[pl.ds(0, times), pl.ds(0, sum(rows) // times)], send.at[i])


def ending(done, lefts, rights, total, out, rest, sems):
    start, size = pieces()[PIECES - 1]
    whole = pltpu.make_async_copy(done.at[pl.ds(0, start)], out.at[pl.ds(0, start)], sems.at[0])
    whole.start()
    at = pl.ds(start, size)
    z = lax.axis_index("replica") // 2
    far = ((z + 2) % 4) * 2
    product(lefts, rights, (far, far + 1), at, rest, total, into=pl.ds(0, size))
    last = pltpu.make_async_copy(rest, out.at[at], sems.at[1])
    last.start()
    whole.wait()
    last.wait()


def body(tokens_in, cotangents, left_root, right_root):
    rows, depth = tokens_in.shape
    columns = right_root.shape[3]
    bf16 = jnp.bfloat16
    vmem, anywhere = pl.BlockSpec(memory_space=pltpu.VMEM), pl.BlockSpec(memory_space=pl.ANY)
    done, lefts, rights, total = pl.pallas_call(
        kernel,
        out_shape=(
            pltpu.VMEM((depth, columns), bf16),
            pltpu.VMEM((8, depth, rows), bf16),
            pltpu.VMEM((8, rows, columns), bf16),
            pltpu.VMEM((sum(GROUPS[-1]), columns), jnp.float32),
        ),
        in_specs=[anywhere] * 4,
        out_specs=(vmem,) * 4,
        scratch_shapes=[
            pltpu.VMEM((depth, depth), bf16),
            pltpu.VMEM((columns, columns), bf16),
            pltpu.VMEM((rows, depth), bf16),
            pltpu.VMEM((8, rows, columns), bf16),
            pltpu.VMEM((depth - sum(GROUPS[-1]), columns), jnp.float32),
            pltpu.SemaphoreType.DMA((2,)),
            pltpu.SemaphoreType.DMA,
            pltpu.SemaphoreType.DMA,
            pltpu.SemaphoreType.DMA((9,)),
            pltpu.SemaphoreType.DMA((8,)),
            pltpu.SemaphoreType.DMA((16,)),
            pltpu.SemaphoreType.DMA((16 * PIECES,)),
            pltpu.SemaphoreType.REGULAR,
            pltpu.SemaphoreType.REGULAR,
        ],
        compiler_params=pltpu.CompilerParams(
            collective_id=0, has_side_effects=True, vmem_limit_bytes=40 << 20
        ),
    )(tokens_in, cotangents, left_root[0], right_root[0, 0])
    update = pl.pallas_call(
        ending,
        out_shape=jax.ShapeDtypeStruct((depth, columns), bf16),
        in_specs=[vmem] * 4,
        out_specs=anywhere,
        scratch_shapes=[
            pltpu.VMEM((sum(GROUPS[-1]), columns), bf16),
            pltpu.SemaphoreType.DMA((2,)),
        ],
        compiler_params=pltpu.CompilerParams(vmem_limit_bytes=20 << 20),
    )(done, lefts, rights, total)
    return update[None]


def solution(mesh):
    placed = (
        P(BOTH, None),
        P(BOTH, None),
        P("expert", None, None),
        P("expert", "replica", None, None),
    )
    return jax.shard_map(
        body, mesh=mesh, in_specs=placed, out_specs=P("expert", None, "replica"), check_vma=False
    )
```
